256 devices in a mesh: facet: 64 (over z, y, core), freq: 4 (over x).
Axes of the slice: x: 4, y: 4, z: 8, core: 2. Of those that a mesh axis runs over, the one named last changes fastest.
Arguments:
- visibilities: bfloat16 [4, 16384, 2, 512], P('freq', 'facet'), may hold values from -6 to 6
- uvw: bfloat16 [4, 16384, 3, 512], P('freq', 'facet'), may hold values from -4 to 4
- facet_of: int32 [4, 16384, 1], P('freq', 'facet'), may hold values from 0 to 63; in each aligned block of 256 rows (0 to 255, 256 to 511, ..., all dimensions but the last counted through in order) at most 16 rows name the same one
- plane_of: int32 [4, 16384], P('freq', 'facet'), may hold values from 0 to 7
- cell_of: int32 [4, 16384], P('freq', 'facet'), may hold values from 0 to 1023
- kernels: bfloat16 [8, 2, 512, 256], replicated, may hold values from -0.25 to 0.25
- centers: float32 [64, 2], replicated, may hold values from -0.4 to 0.4
Outputs:
- images: float32 [64, 512, 512], P('facet', None, 'freq')
The draws below stay inside these ranges and needn't reach their ends.
Inputs may be any that keep to these rules, and one draw needn't show every extreme that they name: `facet_of`: the facet index k is held by index k of the facet axis. In each aligned block of 256 tiles of one group, no facet is named by more than 16 tiles, and in some blocks one facet is named by exactly 16.
All inputs are finite; a program needn't handle non-finite values.
Results may differ from the reference program's by a relative error of at most 0.0095.
Values may be sent and summed in bfloat16 or wider, within the bound.
A program may use at most 128 MiB of HBM per device.

```python
import math
import jax
import jax.numpy as jnp
import numpy as np
from jax import lax

GRID = 512
PSIDE = 16
ROWS = 512
PLANES = 8
TILES_DEV = 256
GROUPS = 4
FACETS = 64
TILES = 16384
CAP = 16
PATCH = 256
CELLS = 1024


def plant(values, own_key, smallest, high):
    longest = values.shape.index(max(values.shape))
    spots = []
    for shift in (0, 1):
        where = [jax.random.randint(jax.random.fold_in(own_key, axis), (), 0, length) for axis, length in enumerate(values.shape)]
        where[longest] = (where[longest] + shift) % values.shape[longest]
        spots.append(tuple(where))
    return values.at[spots[0]].set(smallest).at[spots[1]].set(high)


def block_scale(own_key, shape, split, smallest, top_value):
    loudness, own = 1.0, jax.random.fold_in(own_key, 6)
    for position, shards_of in split:
        heights = jnp.exp(jax.random.uniform(jax.random.fold_in(own, position), (shards_of,), jnp.float32, smallest / len(split), top_value / len(split)))
        loudness = loudness * jnp.repeat(heights, shape[position] // shards_of).reshape([-1 if axis == position else 1 for axis in range(len(shape))])
    return loudness


def shared_out(stream_key, own, number, rows, amount, top, bound, lean):
    ranking = jax.random.permutation(stream_key, amount)
    packed, ordinary = shares(amount, rows * top, bound, lean, True), shares(amount, rows * top, bound, lean, False)
    places = jnp.arange(amount)

    def named(lengths, turn):
        used = int((lengths > 0).sum())
        fixed = max(1, used // 4)
        passed = fixed + (places - fixed + turn * (used - fixed)) % max(1, amount - fixed)
        return jnp.zeros((amount,), jnp.int32).at[ranking[jnp.where(places < fixed, places, passed)]].set(jnp.asarray(lengths, jnp.int32))

    lengths = jnp.where(number % 4 == 0, named(packed, number // 4), named(ordinary, number - number // 4 - 1))
    mixed = jax.random.permutation(jax.random.fold_in(own, 3), amount)
    giver, receiver = mixed[0:amount // 2 * 2:2], mixed[1:amount // 2 * 2:2]
    room = jnp.minimum(lengths[giver] - 1, bound - lengths[receiver]) // 2
    room = jnp.where((giver == ranking[0]) | (receiver == ranking[0]) | (lengths[receiver] == 0), 0, jnp.maximum(room, 0))
    passed = jax.random.randint(jax.random.fold_in(own, 4), (amount // 2,), 0, 1 << 20) % (room + 1)
    lengths = lengths.at[giver].add(-passed).at[receiver].add(passed)
    members = jnp.searchsorted(jnp.cumsum(lengths), jnp.arange(rows * top), side="right").astype(jnp.int32)
    listing = members.reshape(top, rows).T
    listing = listing[jax.random.permutation(jax.random.fold_in(own, 1), rows)]
    turn = jax.random.randint(jax.random.fold_in(own, 2), (rows, 1), 0, top)
    return jnp.take_along_axis(listing, (jnp.arange(top)[None, :] + turn) % top, axis=1)


def shares(count, total, most, skew, full):
    weights = [(1 << 20) // math.isqrt(standing ** skew) + 1 for standing in range(1, count + 1)]
    largest = most if full else min(most, max(-(-total // count), total * weights[0] // sum(weights)))
    least = 1 if total - largest >= count - 1 else 0
    holding, surplus = [largest] + [least] * (count - 1), total - largest - least * (count - 1)
    while surplus > 0:
        free = [i for i in range(1, count) if holding[i] < largest] or [i for i in range(1, count) if holding[i] < most]
        pool, budget = sum([weights[i] for i in free]), surplus
        for i in free:
            more = min(most - holding[i], max(1, budget * weights[i] // pool), surplus)
            holding[i] = holding[i] + more
            surplus = surplus - more
    return np.array(holding)


def scatter_about(key, extent, spread, bound, cuts=(), kind=jnp.bfloat16):
    array = jax.random.normal(key, extent, jnp.float32) * spread
    if len(cuts) > 0:
        array = block_scale(key, extent, cuts, -0.22, 0.18) * array
    return jnp.clip(array, min=-bound, max=bound).astype(kind)


def setup_inputs(seed: int = 0) -> dict:
    seeds = jax.random.split(jax.random.key(seed), 8)
    visibilities = scatter_about(seeds[0], (GROUPS, TILES, 2, ROWS), 1.0, 6.0, ((0, 4), (1, 64)))
    uvw = jnp.clip(jax.random.uniform(seeds[1], (GROUPS, TILES, 3, ROWS), jnp.float32, -4.0, 4.0) * block_scale(seeds[1], (GROUPS, TILES, 3, ROWS), ((0, 4), (1, 64)), -0.4, 0.0), -4.0, 4.0).astype(jnp.bfloat16)
    facet_of_keys = jax.random.split(jax.random.fold_in(seeds[2], 1), GROUPS * TILES // TILES_DEV)
    facet_of_turns = jax.random.permutation(jax.random.fold_in(seeds[2], 3), GROUPS * TILES // TILES_DEV)
    facet_of = jax.vmap(lambda own, number: shared_out(jax.random.fold_in(seeds[2], 2), own, number, TILES_DEV, FACETS, 1, CAP, 2))(facet_of_keys, facet_of_turns).reshape((GROUPS, TILES, 1))
    plane_of = plant(jax.random.randint(seeds[3], (GROUPS, TILES), 0, PLANES), jax.random.fold_in(seeds[3], 1), 0, PLANES - 1).astype(jnp.int32)
    cell_of = plant(jax.random.randint(seeds[4], (GROUPS, TILES), 0, CELLS), jax.random.fold_in(seeds[4], 1), 0, CELLS - 1).astype(jnp.int32)
    kernels = scatter_about(seeds[5], (PLANES, 2, ROWS, PATCH), ROWS ** -0.5, 0.25)
    centers = jnp.clip(jax.random.uniform(seeds[6], (FACETS, 2), jnp.float32, -0.4, 0.4), -0.4, 0.4)
    return {"visibilities": visibilities, "uvw": uvw, "facet_of": facet_of, "plane_of": plane_of, "cell_of": cell_of, "kernels": kernels, "centers": centers}


def dft_tables(length):
    indices = jnp.arange(length, dtype=jnp.int32)
    products_mod = indices[:, None] * indices[None, :] % length
    angle_table = products_mod.astype(jnp.float32) * (2.0 * jnp.pi / length)
    norm_scale = 1.0 / jnp.sqrt(jnp.float32(length))
    table_real = (jnp.cos(angle_table) * norm_scale).astype(jnp.bfloat16)
    table_imag = (jnp.sin(angle_table) * norm_scale).astype(jnp.bfloat16)
    return (table_real, table_imag)

def rotate_tiles(vis_pair, coords, sky_pos):
    l_coord = sky_pos[:, 0:1]
    m_coord = sky_pos[:, 1:2]
    w_term = jnp.sqrt(1.0 - l_coord * l_coord - m_coord * m_coord) - 1.0
    coords = coords.astype(jnp.float32)
    phase_angle = 2.0 * jnp.pi * (l_coord * coords[:, 0] + m_coord * coords[:, 1] + w_term * coords[:, 2])
    cosine = jnp.cos(phase_angle)
    sine_part = jnp.sin(phase_angle)
    real_part = vis_pair[:, 0].astype(jnp.float32)
    imag_part = vis_pair[:, 1].astype(jnp.float32)
    rot_real = (real_part * cosine + imag_part * sine_part).astype(jnp.bfloat16)
    rot_imag = (imag_part * cosine - real_part * sine_part).astype(jnp.bfloat16)
    return (rot_real, rot_imag)

def reference(visibilities, uvw, facet_of, plane_of, cell_of, kernels, centers):
    facet_count = centers.shape[0]
    row_count = visibilities.shape[3]
    nblocks = GRID // PSIDE
    ncells = nblocks * nblocks
    tile_block = 64
    table_real, table_imag = dft_tables(GRID)
    table_both = jnp.concatenate([table_real, table_imag], axis=1).astype(jnp.float32)
    kern_full = kernels.astype(jnp.float32)
    summed = jnp.zeros((facet_count, 2, GRID, GRID), jnp.float32)
    for group in range(visibilities.shape[0]):
        target = facet_of[group, :, 0]
        sky_rows = centers[target]
        rot_real, rot_imag = rotate_tiles(visibilities[group], uvw[group], sky_rows)

        def grid_block(pieces):
            block_real, block_imag, block_planes = pieces
            chosen = kern_full[block_planes]
            left_real = block_real.astype(jnp.float32)
            left_imag = block_imag.astype(jnp.float32)
            patch_real = jnp.einsum('tr,trq->tq', left_real, chosen[:, 0]) - jnp.einsum('tr,trq->tq', left_imag, chosen[:, 1])
            patch_imag = jnp.einsum('tr,trq->tq', left_real, chosen[:, 1]) + jnp.einsum('tr,trq->tq', left_imag, chosen[:, 0])
            return jnp.concatenate([patch_real, patch_imag], axis=1).astype(jnp.bfloat16)
        patches = lax.map(grid_block, (rot_real.reshape(-1, tile_block, row_count), rot_imag.reshape(-1, tile_block, row_count), plane_of[group].reshape(-1, tile_block)))
        patches = patches.reshape(-1, 2 * PSIDE * PSIDE)
        keys = (target * ncells + cell_of[group]).astype(jnp.int32)
        blocks = jax.ops.segment_sum(patches.astype(jnp.float32), keys, num_segments=facet_count * ncells).astype(jnp.bfloat16)
        grids = blocks.reshape(facet_count, nblocks, nblocks, 2, PSIDE, PSIDE)
        grids = grids.transpose(0, 3, 1, 4, 2, 5).reshape(facet_count, 2 * GRID, GRID)

        def half_transform(one_grid):
            product = jnp.dot(one_grid.astype(jnp.float32), table_both)
            half_real = product[:GRID, :GRID] - product[GRID:, GRID:]
            half_imag = product[:GRID, GRID:] + product[GRID:, :GRID]
            return jnp.stack([half_real, half_imag]).astype(jnp.bfloat16)
        partial_value = lax.map(half_transform, grids)
        partial_value = lax.optimization_barrier(partial_value)
        summed = summed + partial_value.astype(jnp.float32)
    halves = lax.optimization_barrier(summed.astype(jnp.bfloat16))

    def finish(one_half):
        right_side = jnp.concatenate([one_half[0], -one_half[1]], axis=0).astype(jnp.float32)
        return jnp.dot(table_both, right_side)
    return lax.map(finish, halves)
```

```python
import functools

import jax
import jax.numpy as jnp
import numpy as np
from jax import lax
from jax.experimental import pallas as pl
from jax.experimental.pallas import tpu as pltpu
from jax.sharding import PartitionSpec as P

MESH = pl.DeviceIdType.MESH
F32, BF16 = jnp.float32, jnp.bfloat16
SLOTS = 16
PU_SETS = ((0, 8, 4, 12), (1, 15, 7, 9), (2, 14, 6, 10), (3, 13, 5, 11))
CHUNKS = 4
SINE = (6.283185159611163, -41.34165492934347, 81.60099819261225, -76.54965682060198, 39.53581371130458)


def constants():
    perm = np.zeros((512, 512))
    twist = np.zeros((CHUNKS, 2, 32, 128))
    mix = np.zeros((CHUNKS, 64, 256))
    last = np.zeros((4, 16, CHUNKS, 4, 4, 4))
    ones = np.arange(32)
    pv = np.arange(16)
    j2 = np.arange(16)
    for h, pus in enumerate(PU_SETS):
        for i, pu in enumerate(pus):
            for c in range(2):
                for v in range(16):
                    perm[c * 256 + pu * 16 + v, h * 128 + c * 64 + i * 16 + v] = 1
                angle = 2 * np.pi * pu * ones / 512
                lanes = slice(c * 64 + i * 16, c * 64 + i * 16 + 16)
                twist[h, 0, :, lanes] = np.cos(angle)[:, None]
                twist[h, 1, :, lanes] = np.sin(angle)[:, None]
        if h == 0:
            outputs = [((0, 1, 0),), ((1, 1, 0),), ((2, 1, 0), (3, 1, 0)), ((2, 0, 1), (3, 0, -1))]
            weights = [np.ones(16), np.cos(np.pi * j2), np.cos(2 * np.pi * 4 * j2 / 16), -np.sin(2 * np.pi * 4 * j2 / 16)]
        else:
            outputs = [((0, 1, 0), (1, 1, 0)), ((0, 0, 1), (1, 0, -1)), ((2, 1, 0), (3, 1, 0)), ((2, 0, 1), (3, 0, -1))]
            weights = []
            for a in (pus[0], pus[2]):
                weights += [np.cos(2 * np.pi * a * j2 / 16), -np.sin(2 * np.pi * a * j2 / 16)]
        for o in range(4):
            for k2 in range(16):
                row = (k2 // 4) * 16 + o * 4 + k2 % 4
                cos, sin = np.cos(2 * np.pi * pv * k2 / 16), np.sin(2 * np.pi * pv * k2 / 16)
                for i, re, im in outputs[o]:
                    on_re = re * cos + im * sin
                    on_im = -re * sin + im * cos
                    at = i * 16
                    mix[h, row, at : at + 16] += on_re
                    mix[h, row, 64 + at : 64 + at + 16] += on_im
                    mix[h, row, 128 + at : 128 + at + 16] += on_im
                    mix[h, row, 192 + at : 192 + at + 16] -= on_re
            for k in range(4):
                last[k, :, h, :, o, k] = (weights[o] / 512)[:, None]
    inner = 2 * np.pi * ones[:, None] * np.tile(pv, 8)[None, :] / 512
    inner = np.stack([np.cos(inner), np.sin(inner)])
    return (
        perm.astype(BF16),
        twist.astype(np.float32),
        inner.astype(np.float32),
        mix.astype(BF16),
        last.reshape(64, 256).astype(BF16),
    )


def sine(turns):
    turns = turns - 0.25
    turns = turns - jnp.floor(turns + 0.5)
    y = 0.25 - jnp.abs(turns)
    y2 = y * y
    total = F32(SINE[4])
    for c in SINE[3::-1]:
        total = total * y2 + F32(c)
    return total * y


def cosine(turns):
    return sine(turns + 0.25)


def iota(shape, dim, kind=jnp.int32):
    return lax.broadcasted_iota(jnp.int32, shape, dim).astype(kind)


def dot(a, b):
    return jnp.dot(a, b, preferred_element_type=F32)


def dot_nt(a, b):
    return lax.dot_general(a, b, (((1,), (1,)), ((), ())), preferred_element_type=F32)


def kernel(peers, groups, vis, uvw, fac, pla, cel, ker, cen, perm, twist, inner, mix, last, out,
           k_v, cols, lhs, send, recv, csend, crecv, ucs, left, xy, pq, xsend, xrecv,
           ksem, ssem, rsem, cssem, crsem, xssem, xrsem):
    me = lax.axis_index("facet")
    fq = lax.axis_index("freq")

    barrier = pltpu.get_barrier_semaphore()

    @pl.loop(1, peers)
    def _(i):
        pl.semaphore_signal(barrier, inc=1, device_id={"facet": lax.rem(me + i, peers)}, device_id_type=MESH)

    @pl.loop(1, groups)
    def _(i):
        pl.semaphore_signal(barrier, inc=1, device_id={"freq": lax.rem(fq + i, groups)}, device_id_type=MESH)

    loads = []
    for p in range(8):
        for c in range(2):
            copy = pltpu.make_async_copy(ker.at[p, c], k_v.at[pl.ds(512 * p, 512), pl.ds(256 * c, 256)], ksem)
            copy.start()
            loads.append(copy)

    target = fac[...]
    dest = (iota((64, 256), 0) == target)
    dest_b = dest.astype(F32).astype(BF16)
    tri = (iota((256, 256), 0) < iota((256, 256), 1)).astype(F32).astype(BF16)
    before = dot(dest_b, tri)
    rank = jnp.sum(jnp.where(dest, before, 0.0), axis=0, keepdims=True).astype(jnp.int32)
    slot = target * SLOTS + rank

    cells = cel[...]
    spot = lax.rem(me, 8) * SLOTS + rank
    here = iota((128, 256), 0) == spot
    high = jnp.where(here, (cells // 32).astype(F32), 0.0).astype(BF16)
    low = jnp.where(here, lax.rem(cells, 32).astype(F32), 0.0).astype(BF16)
    rows = dot_nt(dest_b, high) * 32.0 + dot_nt(dest_b, low)
    csend[...] = rows.reshape(64, 1, 128)

    eye = iota((256, 256), 0) == iota((256, 256), 1)
    target_col = jnp.sum(jnp.where(eye, target.astype(F32), 0.0), axis=1, keepdims=True)
    plane_col = jnp.sum(jnp.where(eye, pla[...].astype(F32), 0.0), axis=1, keepdims=True)
    mine = target_col == iota((256, 64), 1, F32)
    l_col = jnp.sum(jnp.where(mine, cen[0:1, :], 0.0), axis=1, keepdims=True)
    m_col = jnp.sum(jnp.where(mine, cen[1:2, :], 0.0), axis=1, keepdims=True)
    l_all = jnp.broadcast_to(l_col, (256, 128))
    m_all = jnp.broadcast_to(m_col, (256, 128))
    cols[0] = l_all
    cols[1] = m_all
    cols[2] = jnp.sqrt(1.0 - l_all * l_all - m_all * m_all) - 1.0
    cols[3] = jnp.broadcast_to(plane_col, (256, 128))

    @pl.loop(0, 16)
    def _(b):
        at = pl.ds(pl.multiple_of(b * 16, 16), 16)

        def wide(n):
            return jnp.concatenate([cols[n, at, :]] * 4, axis=1)

        turns = wide(0) * uvw[0, at, :].astype(F32) + wide(1) * uvw[1, at, :].astype(F32) + wide(2) * uvw[2, at, :].astype(F32)
        cos, sin = cosine(turns), sine(turns)
        re, im = vis[0, at, :].astype(F32), vis[1, at, :].astype(F32)
        new_re = (re * cos + im * sin).astype(BF16)
        new_im = (im * cos - re * sin).astype(BF16)
        plane = wide(3)
        lower = pl.ds(pl.multiple_of(b * 16 + 256, 16), 16)
        for p in range(8):
            keep = (plane == p).astype(F32).astype(BF16)
            lhs[at, 512 * p : 512 * p + 512] = new_re * keep
            lhs[lower, 512 * p : 512 * p + 512] = new_im * keep

    for copy in loads:
        copy.wait()
    with_re = dot(lhs[...], k_v[:, :256])
    with_im = dot(lhs[...], k_v[:, 256:])
    patch = jnp.concatenate([with_re[:256] - with_im[256:], with_im[:256] + with_re[256:]], axis=1).astype(BF16)
    patch = dot(patch, perm[...]).astype(BF16)
    pick = (iota((1024, 256), 0) == slot).astype(F32).astype(BF16)

    pl.semaphore_wait(barrier, peers - 1 + groups - 1)

    @pl.loop(1, peers)
    def _(i):
        d = lax.rem(me + i, peers)
        pltpu.make_async_remote_copy(csend.at[d], crecv.at[me], cssem, crsem, device_id={"facet": d}, device_id_type=MESH).start()

    for h in range(CHUNKS):
        block = dot(pick, patch[:, 128 * h : 128 * h + 128]).astype(BF16)
        send[h] = block.reshape(64, SLOTS, 128)

        @pl.loop(1, peers)
        def _(i):
            d = lax.rem(me + i, peers)
            pltpu.make_async_remote_copy(send.at[h, d], recv.at[h, me], ssem, rsem.at[h], device_id={"facet": d}, device_id_type=MESH).start()

        recv[h, me] = send[h, me]
    crecv[me] = csend[me]

    some = pl.ds(0, peers - 1)
    pltpu.make_async_copy(csend.at[some], crecv.at[some], crsem).wait()
    for g in range(8):
        cell = jnp.sum(crecv[8 * g : 8 * g + 8], axis=0)
        bu = jnp.floor(cell * (1.0 / 32.0))
        bv = cell - 32.0 * bu
        lanes = slice(128 * g, 128 * g + 128)
        count = iota((32, 128), 0, F32) * (1.0 / 32.0)
        for n, turns in enumerate((count * bu, count * bv)):
            ucs[2 * n, :, lanes] = cosine(turns)
            ucs[2 * n + 1, :, lanes] = sine(turns)

    @pl.loop(0, 32)
    def _(j):
        uc, us = ucs[0, pl.ds(j, 1), :], ucs[1, pl.ds(j, 1), :]
        vc, vs = ucs[2], ucs[3]
        left[pl.ds(pl.multiple_of(j * 32, 32), 32), :] = (uc * vc - us * vs).astype(BF16)
        left[pl.ds(pl.multiple_of(j * 32 + 1024, 32), 32), :] = (us * vc + uc * vs).astype(BF16)

    for h in range(CHUNKS):
        pltpu.make_async_copy(send.at[h, some], recv.at[h, some], rsem.at[h]).wait()
        xy[...] = dot(left[...], recv[h].reshape(1024, 128))
        ec, es = inner[0], inner[1]

        @pl.loop(0, 32)
        def _(j):
            at = pl.ds(pl.multiple_of(j * 32, 32), 32)
            x, y = xy[at, :], xy[pl.ds(pl.multiple_of(j * 32 + 1024, 32), 32), :]
            dc, ds = twist[h, 0, pl.ds(j, 1), :], twist[h, 1, pl.ds(j, 1), :]
            tc, ts = dc * ec - ds * es, ds * ec + dc * es
            pq[at, 0:128] = (x * tc - y * ts).astype(BF16)
            pq[at, 128:256] = (y * tc + x * ts).astype(BF16)

        xsend[h] = dot_nt(mix[h], pq[...]).astype(BF16).reshape(4, 16, 1024)

        @pl.loop(1, groups)
        def _(i):
            d = lax.rem(fq + i, groups)
            pltpu.make_async_remote_copy(xsend.at[h, d], xrecv.at[h, fq], xssem, xrsem.at[h], device_id={"freq": d}, device_id_type=MESH).start()

        xrecv[h, fq] = xsend[h, fq]

    for h in range(CHUNKS):
        few = pl.ds(0, groups - 1)
        pltpu.make_async_copy(xsend.at[h, few], xrecv.at[h, few], xrsem.at[h]).wait()
    image = dot(last[...], xrecv[...].reshape(256, 1024))
    for a in range(32):
        out[:, a, :] = jnp.concatenate([image[16 * k : 16 * k + 16, 32 * a : 32 * a + 32] for k in range(4)], axis=1)

    pltpu.make_async_copy(csend.at[some], crecv.at[some], cssem).wait()
    for h in range(CHUNKS):
        pltpu.make_async_copy(send.at[h, some], recv.at[h, some], ssem).wait()
        few = pl.ds(0, groups - 1)
        pltpu.make_async_copy(xsend.at[h, few], xrecv.at[h, few], xssem).wait()


def solution(mesh):
    peers, groups = mesh.shape["facet"], mesh.shape["freq"]
    consts = constants()

    def shards(visibilities, uvw, facet_of, plane_of, cell_of, kernels, centers):
        vis = jnp.transpose(visibilities[0], (1, 0, 2))
        coords = jnp.transpose(uvw[0], (1, 0, 2))
        vmem = pl.BlockSpec(memory_space=pltpu.VMEM)
        dma = pltpu.SemaphoreType.DMA
        image = pl.pallas_call(
            functools.partial(kernel, peers, groups),
            out_shape=jax.ShapeDtypeStruct((16, 32, 128), F32),
            in_specs=[vmem] * 5 + [pl.BlockSpec(memory_space=pl.ANY)] + [vmem] * 6,
            out_specs=vmem,
            scratch_shapes=[
                pltpu.VMEM((4096, 512), BF16),
                pltpu.VMEM((4, 256, 128), F32),
                pltpu.VMEM((512, 4096), BF16),
                pltpu.VMEM((CHUNKS, 64, SLOTS, 128), BF16),
                pltpu.VMEM((CHUNKS, 64, SLOTS, 128), BF16),
                pltpu.VMEM((64, 1, 128), F32),
                pltpu.VMEM((64, 1, 128), F32),
                pltpu.VMEM((4, 32, 1024), F32),
                pltpu.VMEM((2048, 1024), BF16),
                pltpu.VMEM((2048, 128), F32),
                pltpu.VMEM((1024, 256), BF16),
                pltpu.VMEM((CHUNKS, 4, 16, 1024), BF16),
                pltpu.VMEM((CHUNKS, 4, 16, 1024), BF16),
                dma, dma, dma((CHUNKS,)), dma, dma, dma, dma((CHUNKS,)),
            ],
            compiler_params=pltpu.CompilerParams(collective_id=0, has_side_effects=True),
        )(vis, coords, facet_of.reshape(1, -1), plane_of, cell_of, kernels, centers.T, *[jnp.asarray(c) for c in consts])
        return image.reshape(1, 512, 128)

    in_specs = (
        P("freq", "facet", None, None),
        P("freq", "facet", None, None),
        P("freq", "facet", None),
        P("freq", "facet"),
        P("freq", "facet"),
        P(),
        P(),
    )
    return jax.shard_map(shards, mesh=mesh, in_specs=in_specs, out_specs=P("facet", None, "freq"), check_vma=False)
```

```python
import functools

import jax
import jax.numpy as jnp
import numpy as np
from jax import lax
from jax.experimental import pallas as pl
from jax.experimental.pallas import tpu as pltpu
from jax.sharding import PartitionSpec as P

MESH = pl.DeviceIdType.MESH
F32, BF16 = jnp.float32, jnp.bfloat16
SLOTS = 16
PU_SETS = ((0, 8, 4, 12), (1, 15, 7, 9), (2, 14, 6, 10), (3, 13, 5, 11))
SETS = 4
CHUNKS = ((0,), (1,), (2,), (3,))
AHEAD = 2
ROWS = 512
SINE = (6.283185159611163, -41.34165492934347, 81.60099819261225, -76.54965682060198, 39.53581371130458)


def constants():
    perm = np.zeros((512, 512))
    twist = np.zeros((SETS, 2, 32, 128))
    mix = np.zeros((SETS, 64, 256))
    last = np.zeros((4, 16, SETS, 4, 4))
    ones = np.arange(32)
    pv = np.arange(16)
    j2 = np.arange(16)
    for h, pus in enumerate(PU_SETS):
        for i, pu in enumerate(pus):
            for c in range(2):
                for v in range(16):
                    perm[c * 256 + pu * 16 + v, h * 128 + c * 64 + i * 16 + v] = 1
                angle = 2 * np.pi * pu * ones / 512
                lanes = slice(c * 64 + i * 16, c * 64 + i * 16 + 16)
                twist[h, 0, :, lanes] = np.cos(angle)[:, None]
                twist[h, 1, :, lanes] = np.sin(angle)[:, None]
        if h == 0:
            outputs = [((0, 1, 0),), ((1, 1, 0),), ((2, 1, 0), (3, 1, 0)), ((2, 0, 1), (3, 0, -1))]
            weights = [np.ones(16), np.cos(np.pi * j2), np.cos(2 * np.pi * 4 * j2 / 16), -np.sin(2 * np.pi * 4 * j2 / 16)]
        else:
            outputs = [((0, 1, 0), (1, 1, 0)), ((0, 0, 1), (1, 0, -1)), ((2, 1, 0), (3, 1, 0)), ((2, 0, 1), (3, 0, -1))]
            weights = []
            for a in (pus[0], pus[2]):
                weights += [np.cos(2 * np.pi * a * j2 / 16), -np.sin(2 * np.pi * a * j2 / 16)]
        for o in range(4):
            for k2 in range(16):
                row = (k2 // 4) * 16 + o * 4 + k2 % 4
                cos, sin = np.cos(2 * np.pi * pv * k2 / 16), np.sin(2 * np.pi * pv * k2 / 16)
                for i, re, im in outputs[o]:
                    on_re = re * cos + im * sin
                    on_im = -re * sin + im * cos
                    at = i * 16
                    mix[h, row, at : at + 16] += on_re
                    mix[h, row, 64 + at : 64 + at + 16] += on_im
                    mix[h, row, 128 + at : 128 + at + 16] += on_im
                    mix[h, row, 192 + at : 192 + at + 16] -= on_re
            for k in range(4):
                last[k, :, h, o, k] = weights[o] / 512
    last = last.reshape(64, SETS, 16)
    last = [np.tile(last[:, list(sets)].reshape(64, -1), (1, 4)) for sets in CHUNKS]
    inner = 2 * np.pi * ones[:, None] * np.tile(pv, 8)[None, :] / 512
    inner = np.stack([np.cos(inner), np.sin(inner)])
    return (
        perm.astype(BF16),
        twist.astype(np.float32),
        inner.astype(np.float32),
        mix.astype(BF16),
        np.concatenate(last, axis=1).astype(BF16),
    )


def sine(turns):
    turns = turns - 0.25
    turns = turns - jnp.floor(turns + 0.5)
    y = 0.25 - jnp.abs(turns)
    y2 = y * y
    total = F32(SINE[4])
    for c in SINE[3::-1]:
        total = total * y2 + F32(c)
    return total * y


def cosine(turns):
    return sine(turns + 0.25)


def iota(shape, dim, kind=jnp.int32):
    return lax.broadcasted_iota(jnp.int32, shape, dim).astype(kind)


def dot(a, b):
    return jnp.dot(a, b, preferred_element_type=F32)


def dot_nt(a, b):
    return lax.dot_general(a, b, (((1,), (1,)), ((), ())), preferred_element_type=F32)


def kernel(peers, groups, *refs):
    far, out, near, refs = refs[:12], refs[12], refs[13:24], refs[24:]
    ker = far[11]
    fac, pla, cel, cen, uvw, vis, perm, twist, inner, mix, last = near
    k_v, cols, lhs, csend, crecv, ucs, left, pq, lsem, ksem, cssem, crsem, *rest = refs
    n = len(CHUNKS)
    send, recv, xsend, xrecv = (rest[n * i : n * i + n] for i in range(4))
    ssem, rsem, xssem, xrsem, table = rest[4 * n :]
    me = lax.axis_index("facet")
    fq = lax.axis_index("freq")

    arrive = [pltpu.make_async_copy(a, b, lsem.at[i]) for i, (a, b) in enumerate(zip(far, near))]
    for copy in arrive:
        copy.start()
    loads = []
    for p in range(8):
        for c in range(2):
            copy = pltpu.make_async_copy(ker.at[p, c], k_v.at[pl.ds(512 * p, 512), pl.ds(256 * c, 256)], ksem)
            copy.start()
            loads.append(copy)
    barrier = pltpu.get_barrier_semaphore()

    @pl.loop(1, peers)
    def _(i):
        pl.semaphore_signal(barrier, inc=1, device_id={"facet": lax.rem(me + i, peers)}, device_id_type=MESH)

    @pl.loop(1, groups)
    def _(i):
        pl.semaphore_signal(barrier, inc=1, device_id={"freq": lax.rem(fq + i, groups)}, device_id_type=MESH)

    for copy in arrive[:4]:
        copy.wait()

    target = fac[...]
    dest = (iota((64, 256), 0) == target)
    dest_b = dest.astype(F32).astype(BF16)
    tri = (iota((256, 256), 0) < iota((256, 256), 1)).astype(F32).astype(BF16)
    before = dot(dest_b, tri)
    rank = jnp.sum(jnp.where(dest, before, 0.0), axis=0, keepdims=True).astype(jnp.int32)
    slot = target * SLOTS + rank

    cells = cel[...]
    spot = lax.rem(me, 8) * SLOTS + rank
    here = iota((128, 256), 0) == spot
    high = jnp.where(here, (cells // 32).astype(F32), 0.0).astype(BF16)
    low = jnp.where(here, lax.rem(cells, 32).astype(F32), 0.0).astype(BF16)
    rows = dot_nt(dest_b, high) * 32.0 + dot_nt(dest_b, low)
    csend[...] = rows.reshape(64, 1, 128)

    eye = iota((256, 256), 0) == iota((256, 256), 1)
    target_col = jnp.sum(jnp.where(eye, target.astype(F32), 0.0), axis=1, keepdims=True)
    plane_col = jnp.sum(jnp.where(eye, pla[...].astype(F32), 0.0), axis=1, keepdims=True)
    mine = target_col == iota((256, 64), 1, F32)
    l_col = jnp.sum(jnp.where(mine, cen[0:1, :], 0.0), axis=1, keepdims=True)
    m_col = jnp.sum(jnp.where(mine, cen[1:2, :], 0.0), axis=1, keepdims=True)
    l_all = jnp.broadcast_to(l_col, (256, 128))
    m_all = jnp.broadcast_to(m_col, (256, 128))
    cols[0] = l_all
    cols[1] = m_all
    cols[2] = jnp.sqrt(1.0 - l_all * l_all - m_all * m_all) - 1.0
    cols[3] = jnp.broadcast_to(plane_col, (256, 128))

    arrive[4].wait()
    arrive[5].wait()

    @pl.loop(0, 16)
    def _(b):
        at = pl.ds(pl.multiple_of(b * 16, 16), 16)

        def wide(n):
            return jnp.concatenate([cols[n, at, :]] * 4, axis=1)

        turns = wide(0) * uvw[0, at, :].astype(F32) + wide(1) * uvw[1, at, :].astype(F32) + wide(2) * uvw[2, at, :].astype(F32)
        cos, sin = cosine(turns), sine(turns)
        both = vis[at].astype(F32)
        re, im = both[:, 0, :], both[:, 1, :]
        new_re = (re * cos + im * sin).astype(BF16)
        new_im = (im * cos - re * sin).astype(BF16)
        plane = wide(3)
        lower = pl.ds(pl.multiple_of(b * 16 + 256, 16), 16)
        for p in range(8):
            keep = (plane == p).astype(F32).astype(BF16)
            lhs[at, 512 * p : 512 * p + 512] = new_re * keep
            lhs[lower, 512 * p : 512 * p + 512] = new_im * keep

    pl.semaphore_wait(barrier, peers - 1 + groups - 1)

    @pl.loop(1, peers)
    def _(i):
        d = lax.rem(me + i, peers)
        pltpu.make_async_remote_copy(csend.at[d], crecv.at[me], cssem, crsem, device_id={"facet": d}, device_id_type=MESH).start()

    for copy in arrive[6:] + loads:
        copy.wait()
    with_re = dot(lhs[...], k_v[:, :256])
    with_im = dot(lhs[...], k_v[:, 256:])
    patch = jnp.concatenate([with_re[:256] - with_im[256:], with_im[:256] + with_re[256:]], axis=1).astype(BF16)
    patch = dot(patch, perm[...]).astype(BF16)
    pick = (iota((1024, 256), 0) == slot).astype(F32).astype(BF16)

    def launch(h):
        for i, a in enumerate(CHUNKS[h]):
            block = dot(pick, patch[:, 128 * a : 128 * a + 128]).astype(BF16)
            send[h][:, :, 128 * i : 128 * i + 128] = block.reshape(64, SLOTS, 128)

        @pl.loop(1, peers)
        def _(i):
            d = lax.rem(me + i, peers)
            pltpu.make_async_remote_copy(send[h].at[d], recv[h].at[me], ssem.at[h], rsem.at[h], device_id={"facet": d}, device_id_type=MESH).start()

        recv[h][me] = send[h][me]

    for h in range(AHEAD):
        launch(h)
    crecv[me] = csend[me]

    some = pl.ds(0, peers - 1)
    pltpu.make_async_copy(csend.at[some], crecv.at[some], crsem).wait()
    for g in range(8):
        cell = jnp.sum(crecv[8 * g : 8 * g + 8], axis=0)
        bu = jnp.floor(cell * (1.0 / 32.0))
        bv = cell - 32.0 * bu
        lanes = slice(128 * g, 128 * g + 128)
        count = iota((32, 128), 0, F32) * (1.0 / 32.0)
        for w, turns in enumerate((count * bu, count * bv)):
            ucs[2 * w, :, lanes] = cosine(turns)
            ucs[2 * w + 1, :, lanes] = sine(turns)

    @pl.loop(0, 32)
    def _(j):
        uc, us = ucs[0, pl.ds(j, 1), :], ucs[1, pl.ds(j, 1), :]
        vc, vs = ucs[2], ucs[3]
        left[pl.ds(pl.multiple_of(j * 32, 32), 32), :] = (uc * vc - us * vs).astype(BF16)
        left[pl.ds(pl.multiple_of(j * 32 + 1024, 32), 32), :] = (us * vc + uc * vs).astype(BF16)

    ec, es = inner[0], inner[1]
    for a in range(SETS):

        @pl.loop(0, 32)
        def _(j):
            at = pl.ds(pl.multiple_of(j * 32, 32), 32)
            dc, ds = twist[a, 0, pl.ds(j, 1), :], twist[a, 1, pl.ds(j, 1), :]
            table[2 * a, at] = dc * ec - ds * es
            table[2 * a + 1, at] = ds * ec + dc * es

    for h, sets in enumerate(CHUNKS):
        pltpu.make_async_copy(send[h].at[some], recv[h].at[some], rsem.at[h]).wait()
        if h + AHEAD < n:
            launch(h + AHEAD)
        for i, a in enumerate(sets):
            block = recv[h][:, :, 128 * i : 128 * i + 128].reshape(1024, 128)
            for b in range(0, 1024, ROWS):
                at = slice(b, b + ROWS)
                x, y = dot(left[at], block), dot(left[b + 1024 : b + 1024 + ROWS], block)
                tc, ts = table[2 * a, at], table[2 * a + 1, at]
                pq[at, 0:128] = (x * tc - y * ts).astype(BF16)
                pq[at, 128:256] = (y * tc + x * ts).astype(BF16)

            xsend[h][:, 16 * i : 16 * i + 16, :] = dot_nt(mix[a], pq[...]).astype(BF16).reshape(4, 16, 1024)

        @pl.loop(1, groups)
        def _(i):
            d = lax.rem(fq + i, groups)
            pltpu.make_async_remote_copy(xsend[h].at[d], xrecv[h].at[fq], xssem.at[h], xrsem.at[h], device_id={"freq": d}, device_id_type=MESH).start()

        xrecv[h][fq] = xsend[h][fq]

    few = pl.ds(0, groups - 1)
    image = 0.0
    start = 0
    for h, sets in enumerate(CHUNKS):
        pltpu.make_async_copy(xsend[h].at[few], xrecv[h].at[few], xrsem.at[h]).wait()
        wide = 64 * len(sets)
        image = image + dot(last[:, start : start + wide], xrecv[h][...].reshape(wide, 1024))
        start += wide
    for a in range(32):
        out[:, a, :] = jnp.concatenate([image[16 * k : 16 * k + 16, 32 * a : 32 * a + 32] for k in range(4)], axis=1)

    pltpu.make_async_copy(csend.at[some], crecv.at[some], cssem).wait()
    for h in range(n):
        pltpu.make_async_copy(send[h].at[some], recv[h].at[some], ssem.at[h]).wait()
        pltpu.make_async_copy(xsend[h].at[few], xrecv[h].at[few], xssem.at[h]).wait()


def solution(mesh):
    peers, groups = mesh.shape["facet"], mesh.shape["freq"]
    consts = constants()
    widths = [len(sets) for sets in CHUNKS]

    def shards(visibilities, uvw, facet_of, plane_of, cell_of, kernels, centers):
        coords = jnp.transpose(uvw[0], (1, 0, 2))
        small = [facet_of.reshape(1, -1), plane_of, cell_of, centers.T, coords, visibilities[0], *[jnp.asarray(c) for c in consts]]
        vmem = pl.BlockSpec(memory_space=pltpu.VMEM)
        dma = pltpu.SemaphoreType.DMA
        image = pl.pallas_call(
            functools.partial(kernel, peers, groups),
            out_shape=jax.ShapeDtypeStruct((16, 32, 128), F32),
            in_specs=[pl.BlockSpec(memory_space=pltpu.HBM)] * 12,
            out_specs=vmem,
            scratch_shapes=[
                *[pltpu.VMEM(a.shape, a.dtype) for a in small],
                pltpu.VMEM((4096, 512), BF16),
                pltpu.VMEM((4, 256, 128), F32),
                pltpu.VMEM((512, 4096), BF16),
                pltpu.VMEM((64, 1, 128), F32),
                pltpu.VMEM((64, 1, 128), F32),
                pltpu.VMEM((4, 32, 1024), F32),
                pltpu.VMEM((2048, 1024), BF16),
                pltpu.VMEM((1024, 256), BF16),
                dma((11,)), dma, dma, dma,
                *[pltpu.VMEM((64, SLOTS, 128 * k), BF16) for k in widths * 2],
                *[pltpu.VMEM((4, 16 * k, 1024), BF16) for k in widths * 2],
                *[dma((len(CHUNKS),))] * 4,
                pltpu.VMEM((2 * SETS, 1024, 128), F32),
            ],
            compiler_params=pltpu.CompilerParams(collective_id=0, has_side_effects=True),
        )(*small, kernels)
        return image.reshape(1, 512, 128)

    in_specs = (
        P("freq", "facet", None, None),
        P("freq", "facet", None, None),
        P("freq", "facet", None),
        P("freq", "facet"),
        P("freq", "facet"),
        P(),
        P(),
    )
    return jax.shard_map(shards, mesh=mesh, in_specs=in_specs, out_specs=P("facet", None, "freq"), check_vma=False)
```

```python
import functools

import jax
import jax.numpy as jnp
import numpy as np
from jax import lax
from jax.experimental import pallas as pl
from jax.experimental.pallas import tpu as pltpu
from jax.sharding import PartitionSpec as P

MESH = pl.DeviceIdType.MESH
F32, BF16 = jnp.float32, jnp.bfloat16
SLOTS = 16
PU_SETS = ((0, 8, 4, 12), (1, 15, 7, 9), (2, 14, 6, 10), (3, 13, 5, 11))
SETS = 4
CHUNKS = ((0,), (1,), (2,), (3,))
AHEAD = 3
ROWS = 512
SINE = (6.283185159611163, -41.34165492934347, 81.60099819261225, -76.54965682060198, 39.53581371130458)


def constants():
    perm = np.zeros((512, 512))
    twist = np.zeros((SETS, 2, 32, 128))
    mix = np.zeros((SETS, 64, 256))
    last = np.zeros((4, 16, SETS, 4, 4))
    ones = np.arange(32)
    pv = np.arange(16)
    j2 = np.arange(16)
    for h, pus in enumerate(PU_SETS):
        for i, pu in enumerate(pus):
            for c in range(2):
                for v in range(16):
                    perm[c * 256 + pu * 16 + v, h * 128 + c * 64 + i * 16 + v] = 1
                angle = 2 * np.pi * pu * ones / 512
                lanes = slice(c * 64 + i * 16, c * 64 + i * 16 + 16)
                twist[h, 0, :, lanes] = np.cos(angle)[:, None]
                twist[h, 1, :, lanes] = np.sin(angle)[:, None]
        if h == 0:
            outputs = [((0, 1, 0),), ((1, 1, 0),), ((2, 1, 0), (3, 1, 0)), ((2, 0, 1), (3, 0, -1))]
            weights = [np.ones(16), np.cos(np.pi * j2), np.cos(2 * np.pi * 4 * j2 / 16), -np.sin(2 * np.pi * 4 * j2 / 16)]
        else:
            outputs = [((0, 1, 0), (1, 1, 0)), ((0, 0, 1), (1, 0, -1)), ((2, 1, 0), (3, 1, 0)), ((2, 0, 1), (3, 0, -1))]
            weights = []
            for a in (pus[0], pus[2]):
                weights += [np.cos(2 * np.pi * a * j2 / 16), -np.sin(2 * np.pi * a * j2 / 16)]
        for o in range(4):
            for k2 in range(16):
                row = (k2 // 4) * 16 + o * 4 + k2 % 4
                cos, sin = np.cos(2 * np.pi * pv * k2 / 16), np.sin(2 * np.pi * pv * k2 / 16)
                for i, re, im in outputs[o]:
                    on_re = re * cos + im * sin
                    on_im = -re * sin + im * cos
                    at = i * 16
                    mix[h, row, at : at + 16] += on_re
                    mix[h, row, 64 + at : 64 + at + 16] += on_im
                    mix[h, row, 128 + at : 128 + at + 16] += on_im
                    mix[h, row, 192 + at : 192 + at + 16] -= on_re
            for k in range(4):
                last[k, :, h, o, k] = weights[o] / 512
    last = last.reshape(64, SETS, 16)
    last = [np.tile(last[:, list(sets)].reshape(64, -1), (1, 4)) for sets in CHUNKS]
    inner = 2 * np.pi * ones[:, None] * np.tile(pv, 8)[None, :] / 512
    inner = np.stack([np.cos(inner), np.sin(inner)])
    return (
        perm.astype(BF16),
        twist.astype(np.float32),
        inner.astype(np.float32),
        mix.astype(BF16),
        np.concatenate(last, axis=1).astype(BF16),
    )


def sine(turns):
    turns = turns - 0.25
    turns = turns - jnp.floor(turns + 0.5)
    y = 0.25 - jnp.abs(turns)
    y2 = y * y
    total = F32(SINE[4])
    for c in SINE[3::-1]:
        total = total * y2 + F32(c)
    return total * y


def cosine(turns):
    return sine(turns + 0.25)


def iota(shape, dim, kind=jnp.int32):
    return lax.broadcasted_iota(jnp.int32, shape, dim).astype(kind)


def dot(a, b):
    return jnp.dot(a, b, preferred_element_type=F32)


def dot_nt(a, b):
    return lax.dot_general(a, b, (((1,), (1,)), ((), ())), preferred_element_type=F32)


def kernel(peers, groups, *refs):
    far, out, near, refs = refs[:12], refs[12], refs[13:24], refs[24:]
    ker = far[11]
    fac, pla, cel, cen, uvw, vis, perm, twist, inner, mix, last = near
    k_v, cols, lhs, csend, crecv, ucs, left, pq, lsem, ksem, cssem, crsem, *rest = refs
    n = len(CHUNKS)
    send, recv, xsend, xrecv = (rest[n * i : n * i + n] for i in range(4))
    ssem, rsem, xssem, xrsem, table = rest[4 * n :]
    me = lax.axis_index("facet")
    fq = lax.axis_index("freq")

    arrive = [pltpu.make_async_copy(a, b, lsem.at[i]) for i, (a, b) in enumerate(zip(far, near))]
    for copy in arrive:
        copy.start()
    loads = []
    for p in range(8):
        for c in range(2):
            copy = pltpu.make_async_copy(ker.at[p, c], k_v.at[pl.ds(512 * p, 512), pl.ds(256 * c, 256)], ksem)
            copy.start()
            loads.append(copy)
    barrier = pltpu.get_barrier_semaphore()

    @pl.loop(1, peers)
    def _(i):
        pl.semaphore_signal(barrier, inc=1, device_id={"facet": lax.rem(me + i, peers)}, device_id_type=MESH)

    @pl.loop(1, groups)
    def _(i):
        pl.semaphore_signal(barrier, inc=1, device_id={"freq": lax.rem(fq + i, groups)}, device_id_type=MESH)

    for copy in arrive[:4]:
        copy.wait()

    target = fac[...]
    dest = (iota((64, 256), 0) == target)
    dest_b = dest.astype(F32).astype(BF16)
    tri = (iota((256, 256), 0) < iota((256, 256), 1)).astype(F32).astype(BF16)
    before = dot(dest_b, tri)
    rank = jnp.sum(jnp.where(dest, before, 0.0), axis=0, keepdims=True).astype(jnp.int32)
    slot = target * SLOTS + rank

    cells = cel[...]
    spot = lax.rem(me, 8) * SLOTS + rank
    here = iota((128, 256), 0) == spot
    high = jnp.where(here, (cells // 32).astype(F32), 0.0).astype(BF16)
    low = jnp.where(here, lax.rem(cells, 32).astype(F32), 0.0).astype(BF16)
    rows = dot_nt(dest_b, high) * 32.0 + dot_nt(dest_b, low)
    csend[...] = rows.reshape(64, 1, 128)

    eye = iota((256, 256), 0) == iota((256, 256), 1)
    target_col = jnp.sum(jnp.where(eye, target.astype(F32), 0.0), axis=1, keepdims=True)
    plane_col = jnp.sum(jnp.where(eye, pla[...].astype(F32), 0.0), axis=1, keepdims=True)
    mine = target_col == iota((256, 64), 1, F32)
    l_col = jnp.sum(jnp.where(mine, cen[0:1, :], 0.0), axis=1, keepdims=True)
    m_col = jnp.sum(jnp.where(mine, cen[1:2, :], 0.0), axis=1, keepdims=True)
    l_all = jnp.broadcast_to(l_col, (256, 128))
    m_all = jnp.broadcast_to(m_col, (256, 128))
    cols[0] = l_all
    cols[1] = m_all
    cols[2] = jnp.sqrt(1.0 - l_all * l_all - m_all * m_all) - 1.0
    cols[3] = jnp.broadcast_to(plane_col, (256, 128))

    arrive[4].wait()
    arrive[5].wait()

    @pl.loop(0, 16)
    def _(b):
        at = pl.ds(pl.multiple_of(b * 16, 16), 16)

        def wide(n):
            return jnp.concatenate([cols[n, at, :]] * 4, axis=1)

        turns = wide(0) * uvw[0, at, :].astype(F32) + wide(1) * uvw[1, at, :].astype(F32) + wide(2) * uvw[2, at, :].astype(F32)
        cos, sin = cosine(turns), sine(turns)
        both = vis[at].astype(F32)
        re, im = both[:, 0, :], both[:, 1, :]
        new_re = (re * cos + im * sin).astype(BF16)
        new_im = (im * cos - re * sin).astype(BF16)
        plane = wide(3)
        lower = pl.ds(pl.multiple_of(b * 16 + 256, 16), 16)
        for p in range(8):
            keep = (plane == p).astype(F32).astype(BF16)
            lhs[at, 512 * p : 512 * p + 512] = new_re * keep
            lhs[lower, 512 * p : 512 * p + 512] = new_im * keep

    pl.semaphore_wait(barrier, peers - 1 + groups - 1)

    @pl.loop(1, peers)
    def _(i):
        d = lax.rem(me + i, peers)
        pltpu.make_async_remote_copy(csend.at[d], crecv.at[me], cssem, crsem, device_id={"facet": d}, device_id_type=MESH).start()

    for copy in arrive[6:] + loads:
        copy.wait()
    with_re = dot(lhs[...], k_v[:, :256])
    with_im = dot(lhs[...], k_v[:, 256:])
    patch = jnp.concatenate([with_re[:256] - with_im[256:], with_im[:256] + with_re[256:]], axis=1).astype(BF16)
    patch = dot(patch, perm[...]).astype(BF16)
    pick = (iota((1024, 256), 0) == slot).astype(F32).astype(BF16)

    def launch(h):
        for i, a in enumerate(CHUNKS[h]):
            block = dot(pick, patch[:, 128 * a : 128 * a + 128]).astype(BF16)
            send[h][:, :, 128 * i : 128 * i + 128] = block.reshape(64, SLOTS, 128)

        @pl.loop(1, peers)
        def _(i):
            d = lax.rem(me + i, peers)
            pltpu.make_async_remote_copy(send[h].at[d], recv[h].at[me], ssem.at[h], rsem.at[h], device_id={"facet": d}, device_id_type=MESH).start()

        recv[h][me] = send[h][me]

    for h in range(AHEAD):
        launch(h)
    crecv[me] = csend[me]

    some = pl.ds(0, peers - 1)
    pltpu.make_async_copy(csend.at[some], crecv.at[some], crsem).wait()
    for g in range(8):
        cell = jnp.sum(crecv[8 * g : 8 * g + 8], axis=0)
        bu = jnp.floor(cell * (1.0 / 32.0))
        bv = cell - 32.0 * bu
        lanes = slice(128 * g, 128 * g + 128)
        count = iota((32, 128), 0, F32) * (1.0 / 32.0)
        for w, turns in enumerate((count * bu, count * bv)):
            ucs[2 * w, :, lanes] = cosine(turns)
            ucs[2 * w + 1, :, lanes] = sine(turns)

    @pl.loop(0, 32)
    def _(j):
        uc, us = ucs[0, pl.ds(j, 1), :], ucs[1, pl.ds(j, 1), :]
        vc, vs = ucs[2], ucs[3]
        left[pl.ds(pl.multiple_of(j * 32, 32), 32), :] = (uc * vc - us * vs).astype(BF16)
        left[pl.ds(pl.multiple_of(j * 32 + 1024, 32), 32), :] = (us * vc + uc * vs).astype(BF16)

    ec, es = inner[0], inner[1]
    for a in range(SETS):

        @pl.loop(0, 32)
        def _(j):
            at = pl.ds(pl.multiple_of(j * 32, 32), 32)
            dc, ds = twist[a, 0, pl.ds(j, 1), :], twist[a, 1, pl.ds(j, 1), :]
            table[2 * a, at] = dc * ec - ds * es
            table[2 * a + 1, at] = ds * ec + dc * es

    for h, sets in enumerate(CHUNKS):
        pltpu.make_async_copy(send[h].at[some], recv[h].at[some], rsem.at[h]).wait()
        if h + AHEAD < n:
            launch(h + AHEAD)
        for i, a in enumerate(sets):
            block = recv[h][:, :, 128 * i : 128 * i + 128].reshape(1024, 128)
            for b in range(0, 1024, ROWS):
                at = slice(b, b + ROWS)
                x, y = dot(left[at], block), dot(left[b + 1024 : b + 1024 + ROWS], block)
                tc, ts = table[2 * a, at], table[2 * a + 1, at]
                pq[at, 0:128] = (x * tc - y * ts).astype(BF16)
                pq[at, 128:256] = (y * tc + x * ts).astype(BF16)

            xsend[h][:, 16 * i : 16 * i + 16, :] = dot_nt(mix[a], pq[...]).astype(BF16).reshape(4, 16, 1024)

        @pl.loop(1, groups)
        def _(i):
            d = lax.rem(fq + i, groups)
            pltpu.make_async_remote_copy(xsend[h].at[d], xrecv[h].at[fq], xssem.at[h], xrsem.at[h], device_id={"freq": d}, device_id_type=MESH).start()

        xrecv[h][fq] = xsend[h][fq]

    few = pl.ds(0, groups - 1)
    image = 0.0
    start = 0
    for h, sets in enumerate(CHUNKS):
        pltpu.make_async_copy(xsend[h].at[few], xrecv[h].at[few], xrsem.at[h]).wait()
        wide = 64 * len(sets)
        image = image + dot(last[:, start : start + wide], xrecv[h][...].reshape(wide, 1024))
        start += wide
    out[...] = image

    pltpu.make_async_copy(csend.at[some], crecv.at[some], cssem).wait()
    for h in range(n):
        pltpu.make_async_copy(send[h].at[some], recv[h].at[some], ssem.at[h]).wait()
        pltpu.make_async_copy(xsend[h].at[few], xrecv[h].at[few], xssem.at[h]).wait()


def settle(image, out):
    for a in range(32):
        out[:, a, :] = jnp.concatenate([image[16 * k : 16 * k + 16, 32 * a : 32 * a + 32] for k in range(4)], axis=1)


def solution(mesh):
    peers, groups = mesh.shape["facet"], mesh.shape["freq"]
    consts = constants()
    widths = [len(sets) for sets in CHUNKS]

    def shards(visibilities, uvw, facet_of, plane_of, cell_of, kernels, centers):
        coords = jnp.transpose(uvw[0], (1, 0, 2))
        small = [facet_of.reshape(1, -1), plane_of, cell_of, centers.T, coords, visibilities[0], *[jnp.asarray(c) for c in consts]]
        vmem = pl.BlockSpec(memory_space=pltpu.VMEM)
        dma = pltpu.SemaphoreType.DMA
        image = pl.pallas_call(
            functools.partial(kernel, peers, groups),
            out_shape=jax.ShapeDtypeStruct((64, 1024), F32),
            in_specs=[pl.BlockSpec(memory_space=pltpu.HBM)] * 12,
            out_specs=vmem,
            scratch_shapes=[
                *[pltpu.VMEM(a.shape, a.dtype) for a in small],
                pltpu.VMEM((4096, 512), BF16),
                pltpu.VMEM((4, 256, 128), F32),
                pltpu.VMEM((512, 4096), BF16),
                pltpu.VMEM((64, 1, 128), F32),
                pltpu.VMEM((64, 1, 128), F32),
                pltpu.VMEM((4, 32, 1024), F32),
                pltpu.VMEM((2048, 1024), BF16),
                pltpu.VMEM((1024, 256), BF16),
                dma((11,)), dma, dma, dma,
                *[pltpu.VMEM((64, SLOTS, 128 * k), BF16) for k in widths * 2],
                *[pltpu.VMEM((4, 16 * k, 1024), BF16) for k in widths * 2],
                *[dma((len(CHUNKS),))] * 4,
                pltpu.VMEM((2 * SETS, 1024, 128), F32),
            ],
            compiler_params=pltpu.CompilerParams(collective_id=0, has_side_effects=True),
        )(*small, kernels)
        image = pl.pallas_call(
            settle,
            out_shape=jax.ShapeDtypeStruct((16, 32, 128), F32),
            in_specs=[vmem],
            out_specs=vmem,
        )(image)
        return image.reshape(1, 512, 128)

    in_specs = (
        P("freq", "facet", None, None),
        P("freq", "facet", None, None),
        P("freq", "facet", None),
        P("freq", "facet"),
        P("freq", "facet"),
        P(),
        P(),
    )
    return jax.shard_map(shards, mesh=mesh, in_specs=in_specs, out_specs=P("facet", None, "freq"), check_vma=False)
```
